16 devices in a mesh: dp: 4 (over y, z, core), sp: 4 (over x).
Axes of the slice: x: 4, y: 2, z: 1, core: 2. Of those that a mesh axis runs over, the one named last changes fastest.
The devices are a block of a 4x4x8 slice.
Arguments:
- x: bfloat16 [8192, 4096], P(('dp', 'sp')), parts along dimension 0
- gain: bfloat16 [4096], replicated
- wq: bfloat16 [4096, 4096], replicated
- wk: bfloat16 [4096, 4096], replicated
- wv: bfloat16 [4096, 4096], replicated
- wo: bfloat16 [4096, 4096], replicated
Outputs:
- output: bfloat16 [8192, 4096], P(('dp', 'sp')), parts along dimension 0
There are 4 independent parts. The reference program is written for one: setup_inputs(seed, part) draws one part's arguments, and reference() takes and returns one part's arrays. A program takes and returns all parts, laid end to end along the dimension named above; an argument that names none is the same for every part.
All inputs are finite; a program needn't handle non-finite values.
Results may differ from the reference program's by a relative error of at most 0.012.
Values are sent between devices in bfloat16 or wider.
A program may use at most 768 MiB of HBM per device.

```python
import jax
import jax.numpy as jnp
from jax import lax

ROWS = 2048
D = 4096
HEADS = 16
KV_HEADS = 16
HEAD = 256
THETA = 10000


def setup_inputs(seed: int = 0, part: int = 0) -> dict:
    kx, kn, kq, kk, kv, ko = jax.random.split(jax.random.key(seed), 6)

    def weights(key, rows, columns):
        return jax.random.normal(key, (rows, columns), jnp.float32) * rows**-0.5

    drawn = {
        "x": jax.random.normal(jax.random.fold_in(kx, part), (ROWS, D), jnp.float32),
        "gain": 1 + 0.1 * jax.random.normal(kn, (D,), jnp.float32),
        "wq": 2 * weights(kq, D, HEADS * HEAD),
        "wk": 2 * weights(kk, D, KV_HEADS * HEAD),
        "wv": 4 * weights(kv, D, KV_HEADS * HEAD),
        "wo": weights(ko, HEADS * HEAD, D),
    }
    return {k: v.astype(jnp.bfloat16) for k, v in drawn.items()}


def normed(x, gain):
    wide = x.astype(jnp.float32)
    scale = lax.rsqrt(jnp.mean(wide * wide, -1, keepdims=True) + 1e-6)
    return (wide * scale * gain.astype(jnp.float32)).astype(jnp.bfloat16)


def turned(t, place, theta):
    half = t.shape[-1] // 2
    angle = place.astype(jnp.float32)[:, None] * theta ** (-jnp.arange(half, dtype=jnp.float32) / half)
    cos, sin = jnp.cos(angle)[:, None], jnp.sin(angle)[:, None]
    a, b = t[..., :half].astype(jnp.float32), t[..., half:].astype(jnp.float32)
    return jnp.concatenate([a * cos - b * sin, b * cos + a * sin], -1).astype(jnp.bfloat16)


def matmul(a, w):
    return jnp.dot(a, w, preferred_element_type=jnp.float32).astype(jnp.bfloat16)


def einsum(form, a, b):
    return jnp.einsum(form, a.astype(jnp.float32), b.astype(jnp.float32))


def attention(q, k, v):
    scores = einsum("tgsd,ugd->gstu", q, k) * q.shape[-1] ** -0.5
    token = jnp.arange(q.shape[0])
    scores = jnp.where(token[:, None] >= token, scores, -jnp.inf)
    weights = jax.nn.softmax(scores, -1).astype(jnp.bfloat16)
    return einsum("gstu,ugd->tgsd", weights, v).astype(jnp.bfloat16)


def reference(x, gain, wq, wk, wv, wo):
    a, place = normed(x, gain), jnp.arange(ROWS)
    q = turned(matmul(a, wq).reshape(ROWS, HEADS, HEAD), place, THETA).reshape(ROWS, KV_HEADS, -1, HEAD)
    k = turned(matmul(a, wk).reshape(ROWS, KV_HEADS, HEAD), place, THETA)
    v = matmul(a, wv).reshape(ROWS, KV_HEADS, HEAD)
    seen = attention(q, k, v).reshape(ROWS, HEADS * HEAD)
    return (x.astype(jnp.float32) + jnp.dot(seen, wo, preferred_element_type=jnp.float32)).astype(jnp.bfloat16)
```

```python
import functools

import jax
import jax.numpy as jnp
from jax import lax
from jax.experimental import pallas as pl
from jax.experimental.pallas import tpu as pltpu
from jax.sharding import PartitionSpec as P

HEAD = 256
THETA = 10000
NEG = -1e30
HIDDEN = 2 * NEG
LOG2E = 1.4426950408889634
E = HEAD**-0.5 * LOG2E
VMEM_MAX = 67043328
F32, BF16 = jnp.float32, jnp.bfloat16


def _dot(a, b, ca, cb):
    return lax.dot_general(a, b, (((ca,), (cb,)), ((), ())), preferred_element_type=F32)


def normed(x, gain):
    wide = x.astype(F32)
    scale = lax.rsqrt(jnp.mean(wide * wide, -1, keepdims=True) + 1e-6)
    return (wide * scale * gain.astype(F32)).astype(BF16)


def _attention(a_ref, cos_ref, sin_ref, wq_ref, wk_ref, wv_ref, o_ref,
               q_s, k_s, v_s, rq, rk, rv, oo, ro, ro1, lo, rl, rl1, wbuf, m_s, l_s, acc_s, stage,
               w_sem, st_sem, send_sem, recv_sem):
    me = lax.axis_index("sp")
    heads, own, _ = q_s.shape
    groups = heads // 2
    half = own // 2

    def flags(g):
        p = lax.rem(g, 2) == 0
        lo_dev, hi_dev = me < 2, me >= 2
        either = lambda x, y: (p & x) | (jnp.logical_not(p) & y)
        return dict(
            send_kv=lo_dev, kv_to=jnp.where(p, 1 - me, 3 - me),
            send_q=either(hi_dev, me >= 1), q_to=jnp.where(p, 3 - me, jnp.where(me == 1, 0, 5 - me)),
            send_q2=p & (me == 3),
            get_kv=either(lo_dev, hi_dev), get_q=either(me <= 2, me != 1),
            there_own=either(me <= 2, (me == 0) | (me == 2)), there_kv=either(lo_dev, hi_dev),
            send_o=either(lo_dev, me != 1), o_to=jnp.where(p, 3 - me, jnp.where(me == 0, 1, 5 - me)),
            send_o1=p & (me == 2),
            get_o=either(hi_dev, me >= 1), get_o1=p & (me == 3),
            home_kv=either(me == 1, hi_dev),
        )

    def first_head(g):
        return lax.rem(g, 2) * (heads // 2) + lax.div(g, 2) * 2

    def two(ref, g):
        return ref.at[pl.ds(first_head(g), 2)]

    def two1(ref, g):
        return ref.at[pl.ds(lax.div(g, 2) * 2, 2)]

    def remote(src, dst, kind, rkind, g, to):
        return pltpu.make_async_remote_copy(src_ref=src, dst_ref=dst, send_sem=send_sem.at[kind, g], recv_sem=recv_sem.at[rkind, g],
                                            device_id={"sp": to}, device_id_type=pl.DeviceIdType.MESH)

    def copy(kind, g, f):
        return {
            0: lambda: remote(two(q_s, g), two(rq, g), 0, 0, g, f["q_to"]),
            1: lambda: remote(two(k_s, g), two(rk, g), 1, 1, g, f["kv_to"]),
            2: lambda: remote(two(v_s, g), two(rv, g), 2, 2, g, f["kv_to"]),
            3: lambda: remote(two(oo, g), two(ro, g), 3, 3, g, f["o_to"]),
            4: lambda: remote(two(lo, g), two(rl, g), 4, 4, g, f["o_to"]),
            5: lambda: remote(two(oo, g), two1(ro1, g), 5, 5, g, 3),
            6: lambda: remote(two(lo, g), two1(rl1, g), 6, 6, g, 3),
            7: lambda: remote(two(q_s, g), two(rq, g), 7, 0, g, 2),
        }[kind]()

    barrier = pltpu.get_barrier_semaphore()
    for step in (1, 2, 3):
        pl.semaphore_signal(barrier, inc=1, device_id={"sp": lax.rem(me + step, 4)}, device_id_type=pl.DeviceIdType.MESH)
    pl.semaphore_wait(barrier, 3)

    def head_of(i):
        return first_head(lax.div(i, 2)) + lax.rem(i, 2)

    def weights(t, i):
        w = (wq_ref, wk_ref, wv_ref)[t]
        return pltpu.make_async_copy(w.at[:, pl.ds(pl.multiple_of(head_of(i) * HEAD, HEAD), HEAD)], wbuf.at[t], w_sem.at[t])

    for t in range(3):
        weights(t, 0).start()

    def project(i, _):
        h = head_of(i)
        for t in range(3):
            weights(t, i).wait()
            out = _dot(a_ref[...], wbuf[t], 1, 0).astype(BF16)

            @pl.when(i + 1 < heads)
            def _():
                weights(t, i + 1).start()

            if t < 2:
                wide = out.astype(F32)
                x, y = wide[:, : HEAD // 2], wide[:, HEAD // 2 :]
                cos, sin = cos_ref[...], sin_ref[...]
                (q_s, k_s)[t][h] = jnp.concatenate([x * cos - y * sin, y * cos + x * sin], -1).astype(BF16)
            else:
                v_s[h] = out.T

    def project_group(g, _):
        lax.fori_loop(2 * g, 2 * g + 2, project, None)
        f = flags(g)
        for kind, on in ((0, "send_q"), (7, "send_q2"), (1, "send_kv"), (2, "send_kv")):
            @pl.when(f[on])
            def _():
                copy(kind, g, f).start()

    def reset():
        m_s[...] = jnp.full(m_s.shape, NEG, F32)
        l_s[...] = jnp.zeros(l_s.shape, F32)
        acc_s[...] = jnp.zeros(acc_s.shape, F32)

    def block(q, k, v, keys, queries, masked):
        scores = [_dot(k[j, keys, :], q[j, queries, :], 1, 1) for j in range(2)]
        if masked:
            shape = scores[0].shape
            ok = (lax.broadcasted_iota(jnp.int32, shape, 1) + queries.start) >= (lax.broadcasted_iota(jnp.int32, shape, 0) + keys.start)
            scores = [jnp.where(ok, s, HIDDEN) for s in scores]
        ps, keeps = [], []
        for j, s in enumerate(scores):
            old = m_s[j, :, queries]
            top = jnp.maximum(old, s.max(axis=0, keepdims=True))
            p = jnp.exp2((s - top) * E)
            keep = jnp.exp2((old - top) * E)
            m_s[j, :, queries] = top
            l_s[j, :, queries] = l_s[j, :, queries] * keep + p.sum(axis=0, keepdims=True)
            ps.append(p.astype(BF16))
            keeps.append(keep)
        for j in range(2):
            acc_s[j, :, queries] = acc_s[j, :, queries] * keeps[j] + _dot(v[j, :, keys], ps[j], 1, 0)

    every = slice(0, own)

    def there(g):
        f = flags(g)

        @pl.when(f["get_q"])
        def _():
            copy(0, g, f).wait_recv()

        @pl.when(f["get_kv"])
        def _():
            copy(1, g, f).wait_recv()
            copy(2, g, f).wait_recv()

        @pl.when(f["get_q"])
        def _():
            reset()

            @pl.when(f["there_own"])
            def _():
                block(two(rq, g), two(k_s, g), two(v_s, g), every, every, False)

            @pl.when(f["there_kv"])
            def _():
                block(two(rq, g), two(rk, g), two(rv, g), every, every, False)

            h = first_head(g)
            for j in range(2):
                total = l_s[j]
                oo[h + j] = (acc_s[j] * (1 / total)).astype(BF16)
                lo[h + j] = m_s[j] * E + jnp.log2(total)

        for kind, on in ((3, "send_o"), (4, "send_o"), (5, "send_o1"), (6, "send_o1")):
            @pl.when(f[on])
            def _():
                copy(kind, g, f).start()

    def take(part, sums):
        for j in range(2):
            old, new = m_s[j], sums[j] * (1 / E)
            top = jnp.maximum(old, new)
            keep, add = jnp.exp2((old - top) * E), jnp.exp2((new - top) * E)
            m_s[j] = top
            l_s[j] = l_s[j] * keep + add
            acc_s[j] = acc_s[j] * keep + part[j].astype(F32) * add

    def staged(g):
        slot = lax.rem(g, 2)
        at = pl.multiple_of(first_head(g) * HEAD, 2 * HEAD)
        return pltpu.make_async_copy(stage.at[slot], o_ref.at[:, pl.ds(at, 2 * HEAD)], st_sem.at[slot])

    def home(g):
        f = flags(g)
        reset()
        q, k, v = two(q_s, g), two(k_s, g), two(v_s, g)
        block(q, k, v, slice(0, half), every, True)
        block(q, k, v, slice(half, own), slice(half, own), True)

        @pl.when(f["home_kv"])
        def _():
            block(q, two(rk, g), two(rv, g), every, every, False)

        @pl.when(f["get_o"])
        def _():
            copy(3, g, f).wait_recv()
            copy(4, g, f).wait_recv()
            take(two(ro, g), two(rl, g))

        @pl.when(f["get_o1"])
        def _():
            copy(5, g, f).wait_recv()
            copy(6, g, f).wait_recv()
            take(two1(ro1, g), two1(rl1, g))

        @pl.when(g >= 2)
        def _():
            staged(g - 2).wait()

        for j in range(2):
            stage[lax.rem(g, 2), :, j * HEAD : (j + 1) * HEAD] = (acc_s[j] * (1 / l_s[j])).T.astype(BF16)
        staged(g).start()

    def step(s, _):
        @pl.when(2 * s < groups)
        def _():
            lax.fori_loop(2 * s, 2 * s + 2, project_group, None)

        @pl.when(s < groups)
        def _():
            there(s)

        @pl.when(s >= 1)
        def _():
            home(s - 1)

    lax.fori_loop(0, groups + 1, step, None)
    for g in (groups - 2, groups - 1):
        staged(g).wait()

    def drain(g, _):
        f = flags(g)
        for kind, on in ((0, "send_q"), (7, "send_q2"), (1, "send_kv"), (2, "send_kv"), (3, "send_o"), (4, "send_o"), (5, "send_o1"), (6, "send_o1")):
            @pl.when(f[on])
            def _():
                copy(kind, g, f).wait_send()

    lax.fori_loop(0, groups, drain, None)


def attention(a, cos, sin, wq, wk, wv):
    own, depth = a.shape
    heads = wq.shape[1] // HEAD
    groups = heads // 2
    vmem, hbm = pl.BlockSpec(memory_space=pltpu.VMEM), pl.BlockSpec(memory_space=pl.ANY)
    block = pltpu.VMEM((heads, own, HEAD), BF16)
    turned = pltpu.VMEM((heads, HEAD, own), BF16)
    sums = pltpu.VMEM((heads, 1, own), F32)
    return pl.pallas_call(
        _attention,
        out_shape=jax.ShapeDtypeStruct((own, heads * HEAD), BF16),
        in_specs=[vmem, vmem, vmem, hbm, hbm, hbm],
        out_specs=hbm,
        scratch_shapes=[
            block, block, turned, block, block, turned, turned, turned, pltpu.VMEM((heads // 2, HEAD, own), BF16),
            sums, sums, pltpu.VMEM((heads // 2, 1, own), F32),
            pltpu.VMEM((3, depth, HEAD), BF16),
            pltpu.VMEM((2, 1, own), F32), pltpu.VMEM((2, 1, own), F32), pltpu.VMEM((2, HEAD, own), F32),
            pltpu.VMEM((2, own, 2 * HEAD), BF16),
            pltpu.SemaphoreType.DMA((3,)), pltpu.SemaphoreType.DMA((2,)),
            pltpu.SemaphoreType.DMA((8, groups)), pltpu.SemaphoreType.DMA((8, groups)),
        ],
        compiler_params=pltpu.CompilerParams(collective_id=0, has_side_effects=True, vmem_limit_bytes=VMEM_MAX),
        name="attention",
    )(a, cos, sin, wq, wk, wv)


def _output(o_ref, w_ref, x_ref, y_ref):
    y_ref[...] = (x_ref[...].astype(F32) + _dot(o_ref[...], w_ref[...], 1, 0)).astype(BF16)


def output(o, wo, x):
    own, depth = o.shape
    wide = 256
    return pl.pallas_call(
        _output,
        grid=(wo.shape[1] // wide,),
        in_specs=[pl.BlockSpec((own, depth), lambda n: (0, 0)), pl.BlockSpec((depth, wide), lambda n: (0, n)), pl.BlockSpec((own, wide), lambda n: (0, n))],
        out_specs=pl.BlockSpec((own, wide), lambda n: (0, n)),
        out_shape=jax.ShapeDtypeStruct(x.shape, BF16),
        compiler_params=pltpu.CompilerParams(dimension_semantics=("arbitrary",), vmem_limit_bytes=40 * 2**20),
        cost_estimate=pl.CostEstimate(flops=2 * own * depth * wo.shape[1], bytes_accessed=2 * wo.size + 6 * x.size, transcendentals=0),
        name="output",
    )(o, wo, x)


def solution(mesh):
    def step(x, gain, wq, wk, wv, wo):
        own = x.shape[0]
        place = lax.axis_index("sp") * own + jnp.arange(own)
        angle = place.astype(F32)[:, None] * THETA ** (-jnp.arange(HEAD // 2, dtype=F32) / (HEAD // 2))
        o = attention(normed(x, gain), jnp.cos(angle), jnp.sin(angle), wq, wk, wv)
        return output(o, wo, x)

    tokens, whole = P(("dp", "sp"), None), P(None, None)
    return jax.shard_map(step, mesh=mesh, in_specs=(tokens, P(None), whole, whole, whole, whole), out_specs=tokens, check_vma=False)
```

```python
import functools

import jax
import jax.numpy as jnp
from jax import lax
from jax.experimental import pallas as pl
from jax.experimental.pallas import tpu as pltpu
from jax.sharding import PartitionSpec as P

HEAD = 256
THETA = 10000
NEG = -1e30
HIDDEN = 2 * NEG
LOG2E = 1.4426950408889634
E = HEAD**-0.5 * LOG2E
VMEM_MAX = 67043328
F32, BF16 = jnp.float32, jnp.bfloat16


def _dot(a, b, ca, cb):
    return lax.dot_general(a, b, (((ca,), (cb,)), ((), ())), preferred_element_type=F32)


def _layer(x_ref, gain_ref, freq_ref, wq_ref, wk_ref, wv_ref, wo_ref, y_ref,
           a_s, cos_s, sin_s, q_s, k_s, v_s, rq, rk, rv, ro, ro1, lo, rl, rl1, wbuf, m_s, l_s, acc_s, total_s, stage,
           x_sem, w_sem, wo_sem, st_sem, send_sem, recv_sem):
    me = lax.axis_index("sp")
    own, depth = a_s.shape
    heads = q_s.shape[0]
    groups = heads // 2
    pairs = groups // 2
    half = own // 2
    wide = 2 * HEAD
    blocks = depth // wide

    def flags(g):
        p = lax.rem(g, 2) == 0
        low, high = me < 2, me >= 2
        either = lambda x, y: (p & x) | (jnp.logical_not(p) & y)
        return dict(
            send_kv=low, kv_to=jnp.where(p, 1 - me, 3 - me),
            send_q=either(high, me >= 1), q_to=jnp.where(p, 3 - me, jnp.where(me == 1, 0, 5 - me)),
            send_q2=p & (me == 3),
            get_kv=either(low, high), get_q=either(me <= 2, me != 1),
            there_own=either(me <= 2, (me == 0) | (me == 2)), there_kv=either(low, high),
            send_o=either(low, me != 1), o_to=jnp.where(p, 3 - me, jnp.where(me == 0, 1, 5 - me)),
            send_o1=p & (me == 2),
            get_o=either(high, me >= 1), get_o1=p & (me == 3),
            home_kv=either(me == 1, high),
        )

    def first_head(g):
        return lax.rem(g, 2) * (heads // 2) + lax.div(g, 2) * 2

    def two(ref, g):
        return ref.at[pl.ds(first_head(g), 2)]

    def two1(ref, g):
        return ref.at[pl.ds(lax.div(g, 2) * 2, 2)]

    def columns(g):
        return pl.ds(pl.multiple_of(first_head(g) * HEAD, wide), wide)

    def remote(src, dst, kind, rkind, g, to):
        return pltpu.make_async_remote_copy(src_ref=src, dst_ref=dst, send_sem=send_sem.at[kind, g], recv_sem=recv_sem.at[rkind, g],
                                            device_id={"sp": to}, device_id_type=pl.DeviceIdType.MESH)

    def copy(kind, g, f):
        return {
            0: lambda: remote(two(q_s, g), two(rq, g), 0, 0, g, f["q_to"]),
            1: lambda: remote(two(k_s, g), two(rk, g), 1, 1, g, f["kv_to"]),
            2: lambda: remote(two(v_s, g), two(rv, g), 2, 2, g, f["kv_to"]),
            3: lambda: remote(two(rq, g), two(ro, g), 3, 3, g, f["o_to"]),
            4: lambda: remote(two(lo, g), two(rl, g), 4, 4, g, f["o_to"]),
            5: lambda: remote(two(rq, g), two1(ro1, g), 5, 5, g, 3),
            6: lambda: remote(two(lo, g), two1(rl1, g), 6, 6, g, 3),
            7: lambda: remote(two(q_s, g), two(rq, g), 7, 0, g, 2),
        }[kind]()

    ORDER = [(1, 0), (1, 1), (0, 0), (0, 1), (2, 0), (2, 1)]

    def weights(c, i):
        t, cl = ORDER[i]
        w = (wq_ref, wk_ref, wv_ref)[t]
        return pltpu.make_async_copy(w.at[:, columns(2 * c + cl)], wbuf.at[i % 3], w_sem.at[i % 3])

    def rows_in(r):
        return pltpu.make_async_copy(x_ref.at[pl.ds(r * (own // 4), own // 4)], a_s.at[pl.ds(r * (own // 4), own // 4)], x_sem.at[r])

    for r in range(4):
        rows_in(r).start()
    for i in range(3):
        weights(0, i).start()

    barrier = pltpu.get_barrier_semaphore()
    for n in (1, 2, 3):
        pl.semaphore_signal(barrier, inc=1, device_id={"sp": lax.rem(me + n, 4)}, device_id_type=pl.DeviceIdType.MESH)

    place = (me * own + lax.broadcasted_iota(jnp.int32, cos_s.shape, 0)).astype(F32)
    angle = place * freq_ref[...]
    cos_s[...] = jnp.cos(angle)
    sin_s[...] = jnp.sin(angle)

    tall = 32
    for r in range(4):
        rows_in(r).wait()

        def norm(i, _):
            at = pl.ds(pl.multiple_of(r * (own // 4) + i * tall, tall), tall)
            x = a_s[at, :].astype(F32)
            scale = lax.rsqrt(jnp.mean(x * x, -1, keepdims=True) + 1e-6)
            a_s[at, :] = (x * scale * gain_ref[...].astype(F32)).astype(BF16)

        lax.fori_loop(0, own // 4 // tall, norm, None)

    pl.semaphore_wait(barrier, 3)

    def project(c):
        for i, (t, cl) in enumerate(ORDER):
            g = 2 * c + cl
            h = first_head(g)
            weights(c, i).wait()
            out = _dot(a_s[...], wbuf[i % 3], 1, 0).astype(BF16)
            if i < 3:
                weights(c, i + 3).start()
            else:
                @pl.when(c + 1 < pairs)
                def _():
                    weights(c + 1, i - 3).start()

            for j in range(2):
                part = out[:, j * HEAD : (j + 1) * HEAD]
                if t < 2:
                    full = part.astype(F32)
                    x, y = full[:, : HEAD // 2], full[:, HEAD // 2 :]
                    cos, sin = cos_s[...], sin_s[...]
                    part = jnp.concatenate([x * cos - y * sin, y * cos + x * sin], -1).astype(BF16)
                if t == 1:
                    k_s[h + j] = part
                else:
                    (q_s if t == 0 else v_s)[h + j] = part.T

            f = flags(g)
            for kind, on in {0: ((0, "send_q"), (7, "send_q2")), 1: ((1, "send_kv"),), 2: ((2, "send_kv"),)}[t]:
                @pl.when(f[on])
                def _():
                    copy(kind, g, f).start()

    def reset():
        m_s[...] = jnp.full(m_s.shape, NEG, F32)
        l_s[...] = jnp.zeros(l_s.shape, F32)
        acc_s[...] = jnp.zeros(acc_s.shape, F32)

    def block(q, k, v, keys, queries, masked):
        scores = [_dot(k[j, keys, :], q[j, :, queries], 1, 0) for j in range(2)]
        if masked:
            shape = scores[0].shape
            ok = (lax.broadcasted_iota(jnp.int32, shape, 1) + queries.start) >= (lax.broadcasted_iota(jnp.int32, shape, 0) + keys.start)
            scores = [jnp.where(ok, s, HIDDEN) for s in scores]
        ps, keeps = [], []
        for j, s in enumerate(scores):
            old = m_s[j, :, queries]
            top = jnp.maximum(old, s.max(axis=0, keepdims=True))
            p = jnp.exp2((s - top) * E)
            keep = jnp.exp2((old - top) * E)
            m_s[j, :, queries] = top
            l_s[j, :, queries] = l_s[j, :, queries] * keep + p.sum(axis=0, keepdims=True)
            ps.append(p.astype(BF16))
            keeps.append(keep)
        for j in range(2):
            acc_s[j, :, queries] = acc_s[j, :, queries] * keeps[j] + _dot(v[j, :, keys], ps[j], 1, 0)

    every = slice(0, own)

    def there(g, _):
        f = flags(g)

        @pl.when(f["get_q"])
        def _():
            copy(0, g, f).wait_recv()

        @pl.when(f["get_kv"])
        def _():
            copy(1, g, f).wait_recv()
            copy(2, g, f).wait_recv()

        @pl.when(f["get_q"])
        def _():
            reset()

            @pl.when(f["there_own"])
            def _():
                block(two(rq, g), two(k_s, g), two(v_s, g), every, every, False)

            @pl.when(f["there_kv"])
            def _():
                block(two(rq, g), two(rk, g), two(rv, g), every, every, False)

            h = first_head(g)
            for j in range(2):
                total = l_s[j]
                rq[h + j] = (acc_s[j] * (1 / total)).astype(BF16)
                lo[h + j] = m_s[j] * E + jnp.log2(total)

        for kind, on in ((3, "send_o"), (4, "send_o"), (5, "send_o1"), (6, "send_o1")):
            @pl.when(f[on])
            def _():
                copy(kind, g, f).start()

    def take(part, sums):
        for j in range(2):
            old, new = m_s[j], sums[j] * (1 / E)
            top = jnp.maximum(old, new)
            keep, add = jnp.exp2((old - top) * E), jnp.exp2((new - top) * E)
            m_s[j] = top
            l_s[j] = l_s[j] * keep + add
            acc_s[j] = acc_s[j] * keep + part[j].astype(F32) * add

    def out_weights(g, n):
        slot = lax.rem(g, 3)
        return pltpu.make_async_copy(wo_ref.at[columns(g), pl.ds(pl.multiple_of(n * wide, wide), wide)],
                                     wbuf.at[slot, pl.ds(pl.multiple_of(n * wide, wide), wide)], wo_sem.at[slot, n])

    def fetch_out_weights(g):
        lax.fori_loop(0, blocks, lambda n, _: out_weights(g, n).start(), None)

    def residual(n):
        return pltpu.make_async_copy(x_ref.at[:, pl.ds(pl.multiple_of(n * wide, wide), wide)], stage.at[lax.rem(n, 2)], st_sem.at[lax.rem(n, 2)])

    def start_out():
        for g in range(3):
            fetch_out_weights(g)
        residual(0).start()

        def one(n, _):
            @pl.when(n + 1 < blocks)
            def _():
                residual(n + 1).start()

            residual(n).wait()
            total_s[n] = stage[lax.rem(n, 2)].astype(F32)

        lax.fori_loop(0, blocks, one, None)

    def result(n):
        return pltpu.make_async_copy(stage.at[lax.rem(n, 2)], y_ref.at[:, pl.ds(pl.multiple_of(n * wide, wide), wide)], st_sem.at[lax.rem(n, 2)])

    def home(g, _):
        f = flags(g)
        reset()
        q, k, v = two(q_s, g), two(k_s, g), two(v_s, g)
        block(q, k, v, slice(0, half), every, True)
        block(q, k, v, slice(half, own), slice(half, own), True)

        @pl.when(f["home_kv"])
        def _():
            block(q, two(rk, g), two(rv, g), every, every, False)

        @pl.when(f["get_o"])
        def _():
            copy(3, g, f).wait_recv()
            copy(4, g, f).wait_recv()
            take(two(ro, g), two(rl, g))

        @pl.when(f["get_o1"])
        def _():
            copy(5, g, f).wait_recv()
            copy(6, g, f).wait_recv()
            take(two1(ro1, g), two1(rl1, g))

        for j in range(2):
            a_s[:, j * HEAD : (j + 1) * HEAD] = (acc_s[j] * (1 / l_s[j])).T.astype(BF16)

        def one(n, _):
            out_weights(g, n).wait()
            total_s[n] += _dot(a_s[:, :wide], wbuf[lax.rem(g, 3), pl.ds(pl.multiple_of(n * wide, wide), wide), :], 1, 0)

            @pl.when(g + 3 < groups)
            def _():
                out_weights(g + 3, n).start()

            @pl.when(g == groups - 1)
            def _():
                @pl.when(n >= 2)
                def _():
                    result(n - 2).wait()

                stage[lax.rem(n, 2)] = total_s[n].astype(BF16)
                result(n).start()

        lax.fori_loop(0, blocks, one, None)

    def step(t, _):
        @pl.when(t < pairs)
        def _():
            project(t)

        @pl.when(t == pairs)
        def _():
            start_out()

        lax.fori_loop(jnp.where(t > pairs, t - 2, 0), jnp.where(t < pairs, 0, jnp.where(t == groups, groups, t - 1)), home, None)
        lax.fori_loop(jnp.where(t == 1, 0, t), jnp.where(t == 0, 0, jnp.minimum(t + 1, groups)), there, None)

    lax.fori_loop(0, groups + 1, step, None)
    for n in (blocks - 2, blocks - 1):
        result(n).wait()

    def drain(g, _):
        f = flags(g)
        for kind, on in ((0, "send_q"), (7, "send_q2"), (1, "send_kv"), (2, "send_kv"), (3, "send_o"), (4, "send_o"), (5, "send_o1"), (6, "send_o1")):
            @pl.when(f[on])
            def _():
                copy(kind, g, f).wait_send()

    lax.fori_loop(0, groups, drain, None)


def layer(x, gain, freq, wq, wk, wv, wo):
    own, depth = x.shape
    heads = wq.shape[1] // HEAD
    groups = heads // 2
    vmem, hbm = pl.BlockSpec(memory_space=pltpu.VMEM), pl.BlockSpec(memory_space=pl.ANY)
    block = pltpu.VMEM((heads, own, HEAD), BF16)
    turned = pltpu.VMEM((heads, HEAD, own), BF16)
    sums = pltpu.VMEM((heads, 1, own), F32)
    wide = 2 * HEAD
    return pl.pallas_call(
        _layer,
        out_shape=jax.ShapeDtypeStruct((own, depth), BF16),
        in_specs=[hbm, vmem, vmem, hbm, hbm, hbm, hbm],
        out_specs=hbm,
        scratch_shapes=[
            pltpu.VMEM((own, depth), BF16), pltpu.VMEM((own, HEAD // 2), F32), pltpu.VMEM((own, HEAD // 2), F32),
            turned, block, turned, turned, block, turned, turned, pltpu.VMEM((heads // 2, HEAD, own), BF16),
            sums, sums, pltpu.VMEM((heads // 2, 1, own), F32),
            pltpu.VMEM((3, depth, wide), BF16),
            pltpu.VMEM((2, 1, own), F32), pltpu.VMEM((2, 1, own), F32), pltpu.VMEM((2, HEAD, own), F32),
            pltpu.VMEM((depth // wide, own, wide), F32),
            pltpu.VMEM((2, own, wide), BF16),
            pltpu.SemaphoreType.DMA((4,)), pltpu.SemaphoreType.DMA((3,)), pltpu.SemaphoreType.DMA((3, depth // wide)), pltpu.SemaphoreType.DMA((2,)),
            pltpu.SemaphoreType.DMA((8, groups)), pltpu.SemaphoreType.DMA((8, groups)),
        ],
        compiler_params=pltpu.CompilerParams(collective_id=0, has_side_effects=True, vmem_limit_bytes=VMEM_MAX),
        name="layer",
    )(x, gain, freq, wq, wk, wv, wo)


def solution(mesh):
    def step(x, gain, wq, wk, wv, wo):
        freq = THETA ** (-jnp.arange(HEAD // 2, dtype=F32) / (HEAD // 2))
        return layer(x, gain[None], freq[None], wq, wk, wv, wo)

    tokens, whole = P(("dp", "sp"), None), P(None, None)
    return jax.shard_map(step, mesh=mesh, in_specs=(tokens, P(None), whole, whole, whole, whole), out_specs=tokens, check_vma=False)
```

```python
import jax
import jax.numpy as jnp
import numpy as np
from jax import lax
from jax.experimental import pallas as pl
from jax.experimental.pallas import tpu as pltpu
from jax.sharding import PartitionSpec as P

HEAD = 256
THETA = 10000
NEG = -1e30
HIDDEN = 2 * NEG
LOG2E = 1.4426950408889634
E = HEAD**-0.5 * LOG2E
VMEM_MAX = 67043328
F32, BF16 = jnp.float32, jnp.bfloat16


def _dot(a, b, ca, cb):
    return lax.dot_general(a, b, (((ca,), (cb,)), ((), ())), preferred_element_type=F32)


def _layer(x_ref, gain_ref, freq_ref, wq_ref, wk_ref, wv_ref, wo_ref, y_ref,
           a_s, cos_s, sin_s, q_s, k_s, v_s, rq, rk, rv, ro, ro1, lo, rl, rl1, wbuf, product_s, m_s, l_s, acc_s, total_s, stage,
           x_sem, w_sem, wo_sem, st_sem, send_sem, recv_sem):
    me = lax.axis_index("sp")
    own, depth = a_s.shape
    heads = q_s.shape[0]
    groups = heads // 2
    half = own // 2
    wide = 2 * HEAD
    blocks = depth // wide

    def flags(g):
        p = lax.rem(g, 2) == 0
        low, high = me < 2, me >= 2
        either = lambda x, y: (p & x) | (jnp.logical_not(p) & y)
        return dict(
            send_kv=low, kv_to=jnp.where(p, 1 - me, 3 - me),
            send_q=either(high, me >= 1), q_to=jnp.where(p, 3 - me, jnp.where(me == 1, 0, 5 - me)),
            send_q2=p & (me == 3),
            get_kv=either(low, high), get_q=either(me <= 2, me != 1),
            there_own=either(me <= 2, (me == 0) | (me == 2)), there_kv=either(low, high),
            send_o=either(low, me != 1), o_to=jnp.where(p, 3 - me, jnp.where(me == 0, 1, 5 - me)),
            send_o1=p & (me == 2),
            get_o=either(high, me >= 1), get_o1=p & (me == 3),
            home_kv=either(me == 1, high),
        )

    def first_head(g):
        return lax.rem(g, 2) * (heads // 2) + lax.div(g, 2) * 2

    def two(ref, g):
        return ref.at[pl.ds(first_head(g), 2)]

    def two1(ref, g):
        return ref.at[pl.ds(lax.div(g, 2) * 2, 2)]

    def columns(g):
        return pl.ds(pl.multiple_of(first_head(g) * HEAD, wide), wide)

    def remote(src, dst, kind, rkind, g, to):
        return pltpu.make_async_remote_copy(src_ref=src, dst_ref=dst, send_sem=send_sem.at[kind, g], recv_sem=recv_sem.at[rkind, g],
                                            device_id={"sp": to}, device_id_type=pl.DeviceIdType.MESH)

    def copy(kind, g, f):
        return {
            0: lambda: remote(two(q_s, g), two(rq, g), 0, 0, g, f["q_to"]),
            1: lambda: remote(two(k_s, g), two(rk, g), 1, 1, g, f["kv_to"]),
            2: lambda: remote(two(v_s, g), two(rv, g), 2, 2, g, f["kv_to"]),
            3: lambda: remote(two(rq, g), two(ro, g), 3, 3, g, f["o_to"]),
            4: lambda: remote(two(lo, g), two(rl, g), 4, 4, g, f["o_to"]),
            5: lambda: remote(two(rq, g), two1(ro1, g), 5, 5, g, 3),
            6: lambda: remote(two(lo, g), two1(rl1, g), 6, 6, g, 3),
            7: lambda: remote(two(q_s, g), two(rq, g), 7, 0, g, 2),
        }[kind]()

    Q, K, V = 0, 8, 16
    both = lambda *gs: [t + g for c in range(0, len(gs), 2) for t in (V, K) for g in gs[c : c + 2]]
    projections = [
        both(0, 1, 2, 3, 4, 5, 6, 7) + [0, 1, 2, 3, 4, 5, 6, 7],
        both(0, 1, 2, 3, 4, 5, 6, 7) + [1, 3, 5, 7, 0, 2, 4, 6],
        [1, 0, 3, 2, 5, 4, 7, 6] + both(0, 1, 2, 3, 4, 5, 6, 7),
        [0, 1, 2, 3, 4, 5, 6, 7] + both(0, 1, 2, 3, 4, 5, 6, 7),
    ]
    homes = [[0, 1, 2, 3, 4, 5, 6, 7], [0, 2, 4, 6, 1, 3, 5, 7], [0, 1, 2, 3, 4, 5, 6, 7], [1, 3, 0, 2, 5, 4, 6, 7]]
    J, H, BEGIN = 16, 17, 18
    order = [
        [J] * 16 + [0] + [J] * 8 + [2, BEGIN, H, 4, H, H, 6, H, 1, H, 3, H, 5, H, 7, H],
        [J] * 24 + [0, 2, BEGIN, H, 4, H, H, 6, H, H, H, H, H],
        [J] * 12 + [0, 1] + [J] * 4 + [2, 3] + [J] * 8 + [4, 5, BEGIN, 6, 7] + [H] * 8,
        [J] * 24 + [1, 3, BEGIN, 5, H, 7] + [H] * 7,
    ]
    steps = max(len(o) for o in order)
    order = [o + [19] * (steps - len(o)) for o in order]

    def look(table, i):
        found = 0
        for n in range(len(table[0])):
            here = table[3][n]
            for d in range(3):
                if table[d][n] != table[3][n]:
                    here = jnp.where(me == d, table[d][n], here)
            found = jnp.where(i == n, here, found)
        return found

    def weights(what, slot, w):
        return pltpu.make_async_copy(w.at[:, columns(lax.rem(what, groups))], wbuf.at[slot], w_sem.at[slot])

    def fetch(i):
        what = look(projections, i)
        for t, w in enumerate((wq_ref, wk_ref, wv_ref)):
            @pl.when(lax.div(what, groups) == t)
            def _():
                weights(what, lax.rem(i, 3), w).start()

    def rows_in(r):
        return pltpu.make_async_copy(x_ref.at[pl.ds(r * (own // 4), own // 4)], a_s.at[pl.ds(r * (own // 4), own // 4)], x_sem.at[r])

    for r in range(4):
        rows_in(r).start()
    fetch(jnp.int32(0))

    barrier = pltpu.get_barrier_semaphore()
    for n in (1, 2, 3):
        pl.semaphore_signal(barrier, inc=1, device_id={"sp": lax.rem(me + n, 4)}, device_id_type=pl.DeviceIdType.MESH)

    place = (me * own + lax.broadcasted_iota(jnp.int32, cos_s.shape, 0)).astype(F32)
    angle = place * freq_ref[...]
    cos_s[...] = jnp.cos(angle)
    sin_s[...] = jnp.sin(angle)

    for r in range(4):
        rows_in(r).wait()
        at = slice(r * (own // 4), (r + 1) * (own // 4))
        x = a_s[at, :].astype(F32)
        scale = lax.rsqrt(jnp.mean(x * x, -1, keepdims=True) + 1e-6)
        a_s[at, :] = (a_s[at, :].astype(F32) * scale * gain_ref[...]).astype(BF16)

    for i in (1, 2):
        fetch(jnp.int32(i))
    pl.semaphore_wait(barrier, 3)

    def turned(part):
        full = part.astype(F32)
        x, y = full[:, : HEAD // 2], full[:, HEAD // 2 :]
        cos, sin = cos_s[...], sin_s[...]
        return jnp.concatenate([x * cos - y * sin, y * cos + x * sin], -1).astype(BF16)

    def project(i):
        what = look(projections, i)
        t, g = lax.div(what, groups), lax.rem(what, groups)
        h = first_head(g)
        f = flags(g)
        slot = lax.rem(i, 3)
        weights(what, slot, wq_ref).wait()
        product_s[...] = _dot(a_s[...], wbuf[slot], 1, 0).astype(BF16)

        @pl.when(i + 3 < 3 * groups)
        def _():
            fetch(i + 3)

        @pl.when(t == 0)
        def _():
            for j in range(2):
                q_s[h + j] = turned(product_s[:, j * HEAD : (j + 1) * HEAD]).T
            for kind, on in ((0, "send_q"), (7, "send_q2")):
                @pl.when(f[on])
                def _():
                    copy(kind, g, f).start()

        @pl.when(t == 1)
        def _():
            for j in range(2):
                k_s[h + j] = turned(product_s[:, j * HEAD : (j + 1) * HEAD])

            @pl.when(f["send_kv"])
            def _():
                copy(1, g, f).start()

        @pl.when(t == 2)
        def _():
            for j in range(2):
                v_s[h + j] = product_s[:, j * HEAD : (j + 1) * HEAD].T

            @pl.when(f["send_kv"])
            def _():
                copy(2, g, f).start()

    def reset():
        m_s[...] = jnp.full(m_s.shape, NEG, F32)
        l_s[...] = jnp.zeros(l_s.shape, F32)
        acc_s[...] = jnp.zeros(acc_s.shape, F32)

    def block(q, k, v, keys, queries, masked):
        scores = [_dot(k[j, keys, :], q[j, :, queries], 1, 0) for j in range(2)]
        if masked:
            shape = scores[0].shape
            ok = (lax.broadcasted_iota(jnp.int32, shape, 1) + queries.start) >= (lax.broadcasted_iota(jnp.int32, shape, 0) + keys.start)
            scores = [jnp.where(ok, s, HIDDEN) for s in scores]
        ps, keeps = [], []
        for j, s in enumerate(scores):
            old = m_s[j, :, queries]
            top = jnp.maximum(old, s.max(axis=0, keepdims=True))
            p = jnp.exp2((s - top) * E)
            keep = jnp.exp2((old - top) * E)
            m_s[j, :, queries] = top
            l_s[j, :, queries] = l_s[j, :, queries] * keep + p.sum(axis=0, keepdims=True)
            ps.append(p.astype(BF16))
            keeps.append(keep)
        for j in range(2):
            acc_s[j, :, queries] = acc_s[j, :, queries] * keeps[j] + _dot(v[j, :, keys], ps[j], 1, 0)

    every = slice(0, own)

    def there(g):
        f = flags(g)

        @pl.when(f["get_q"])
        def _():
            copy(0, g, f).wait_recv()

        @pl.when(f["get_kv"])
        def _():
            copy(1, g, f).wait_recv()
            copy(2, g, f).wait_recv()

        @pl.when(f["get_q"])
        def _():
            reset()

            @pl.when(f["there_own"])
            def _():
                block(two(rq, g), two(k_s, g), two(v_s, g), every, every, False)

            @pl.when(f["there_kv"])
            def _():
                block(two(rq, g), two(rk, g), two(rv, g), every, every, False)

            h = first_head(g)
            for j in range(2):
                total = l_s[j]
                rq[h + j] = (acc_s[j] * (1 / total)).astype(BF16)
                lo[h + j] = m_s[j] * E + jnp.log2(total)

        for kind, on in ((3, "send_o"), (4, "send_o"), (5, "send_o1"), (6, "send_o1")):
            @pl.when(f[on])
            def _():
                copy(kind, g, f).start()

    def take(part, sums):
        for j in range(2):
            old, new = m_s[j], sums[j] * (1 / E)
            top = jnp.maximum(old, new)
            keep, add = jnp.exp2((old - top) * E), jnp.exp2((new - top) * E)
            m_s[j] = top
            l_s[j] = l_s[j] * keep + add
            acc_s[j] = acc_s[j] * keep + part[j].astype(F32) * add

    def out_weights(i, n):
        slot = lax.rem(i, 3)
        return pltpu.make_async_copy(wo_ref.at[columns(look(homes, i)), pl.ds(pl.multiple_of(n * wide, wide), wide)],
                                     wbuf.at[slot, pl.ds(pl.multiple_of(n * wide, wide), wide)], wo_sem.at[slot, n])

    def residual(n):
        return pltpu.make_async_copy(x_ref.at[:, pl.ds(pl.multiple_of(n * wide, wide), wide)], stage.at[lax.rem(n, 2)], st_sem.at[lax.rem(n, 2)])

    def start_out():
        residual(0).start()
        for i in range(3):
            lax.fori_loop(0, blocks, lambda n, _: out_weights(i, n).start(), None)

        def one(n, _):
            @pl.when(n + 1 < blocks)
            def _():
                residual(n + 1).start()

            residual(n).wait()
            total_s[n] = stage[lax.rem(n, 2)].astype(F32)

        lax.fori_loop(0, blocks, one, None)

    def result(n):
        return pltpu.make_async_copy(stage.at[lax.rem(n, 2)], y_ref.at[:, pl.ds(pl.multiple_of(n * wide, wide), wide)], st_sem.at[lax.rem(n, 2)])

    def home(i):
        g = look(homes, i)
        f = flags(g)
        reset()
        q, k, v = two(q_s, g), two(k_s, g), two(v_s, g)
        block(q, k, v, slice(0, half), every, True)
        block(q, k, v, slice(half, own), slice(half, own), True)

        @pl.when(f["home_kv"])
        def _():
            block(q, two(rk, g), two(rv, g), every, every, False)

        @pl.when(f["get_o"])
        def _():
            copy(3, g, f).wait_recv()
            copy(4, g, f).wait_recv()
            take(two(ro, g), two(rl, g))

        @pl.when(f["get_o1"])
        def _():
            copy(5, g, f).wait_recv()
            copy(6, g, f).wait_recv()
            take(two1(ro1, g), two1(rl1, g))

        for j in range(2):
            a_s[:, j * HEAD : (j + 1) * HEAD] = (acc_s[j] * (1 / l_s[j])).T.astype(BF16)

        def one(n, _):
            out_weights(i, n).wait()
            total_s[n] += _dot(a_s[:, :wide], wbuf[lax.rem(i, 3), pl.ds(pl.multiple_of(n * wide, wide), wide), :], 1, 0)

            @pl.when(i + 3 < groups)
            def _():
                out_weights(i + 3, n).start()

            @pl.when(i == groups - 1)
            def _():
                @pl.when(n >= 2)
                def _():
                    result(n - 2).wait()

                stage[lax.rem(n, 2)] = total_s[n].astype(BF16)
                result(n).start()

        lax.fori_loop(0, blocks, one, None)

    def step(t, done):
        projected, came = done
        what = look(order, t)

        @pl.when(what == J)
        def _():
            project(projected)

        @pl.when(what < groups)
        def _():
            there(what)

        @pl.when(what == BEGIN)
        def _():
            start_out()

        @pl.when(what == H)
        def _():
            home(came)

        return projected + (what == J).astype(jnp.int32), came + (what == H).astype(jnp.int32)

    lax.fori_loop(0, steps, step, (jnp.int32(0), jnp.int32(0)))
    for n in (blocks - 2, blocks - 1):
        result(n).wait()

    def drain(g, _):
        f = flags(g)
        for kind, on in ((0, "send_q"), (7, "send_q2"), (1, "send_kv"), (2, "send_kv"), (3, "send_o"), (4, "send_o"), (5, "send_o1"), (6, "send_o1")):
            @pl.when(f[on])
            def _():
                copy(kind, g, f).wait_send()

    lax.fori_loop(0, groups, drain, None)


def layer(x, gain, freq, wq, wk, wv, wo):
    own, depth = x.shape
    heads = wq.shape[1] // HEAD
    groups = heads // 2
    vmem, hbm = pl.BlockSpec(memory_space=pltpu.VMEM), pl.BlockSpec(memory_space=pl.ANY)
    block = pltpu.VMEM((heads, own, HEAD), BF16)
    turned = pltpu.VMEM((heads, HEAD, own), BF16)
    sums = pltpu.VMEM((heads, 1, own), F32)
    wide = 2 * HEAD
    return pl.pallas_call(
        _layer,
        out_shape=jax.ShapeDtypeStruct((own, depth), BF16),
        in_specs=[hbm, vmem, vmem, hbm, hbm, hbm, hbm],
        out_specs=hbm,
        scratch_shapes=[
            pltpu.VMEM((own, depth), BF16), pltpu.VMEM((own, HEAD // 2), F32), pltpu.VMEM((own, HEAD // 2), F32),
            turned, block, turned, turned, block, turned, turned, pltpu.VMEM((heads // 2, HEAD, own), BF16),
            sums, sums, pltpu.VMEM((heads // 2, 1, own), F32),
            pltpu.VMEM((3, depth, wide), BF16), pltpu.VMEM((own, wide), BF16),
            pltpu.VMEM((2, 1, own), F32), pltpu.VMEM((2, 1, own), F32), pltpu.VMEM((2, HEAD, own), F32),
            pltpu.VMEM((depth // wide, own, wide), F32),
            pltpu.VMEM((2, own, wide), BF16),
            pltpu.SemaphoreType.DMA((4,)), pltpu.SemaphoreType.DMA((3,)), pltpu.SemaphoreType.DMA((3, depth // wide)), pltpu.SemaphoreType.DMA((2,)),
            pltpu.SemaphoreType.DMA((8, groups)), pltpu.SemaphoreType.DMA((8, groups)),
        ],
        compiler_params=pltpu.CompilerParams(collective_id=0, has_side_effects=True, vmem_limit_bytes=VMEM_MAX),
        name="layer",
    )(x, gain, freq, wq, wk, wv, wo)


def solution(mesh):
    def step(x, gain, wq, wk, wv, wo):
        freq = np.float32(THETA) ** (-np.arange(HEAD // 2, dtype=np.float32) / np.float32(HEAD // 2))
        return layer(x, gain.astype(F32)[None], jnp.asarray(freq)[None], wq, wk, wv, wo)

    tokens, whole = P(("dp", "sp"), None), P(None, None)
    return jax.shard_map(step, mesh=mesh, in_specs=(tokens, P(None), whole, whole, whole, whole), out_specs=tokens, check_vma=False)
```

```python
import jax
import jax.numpy as jnp
import numpy as np
from jax import lax
from jax.experimental import pallas as pl
from jax.experimental.pallas import tpu as pltpu
from jax.sharding import PartitionSpec as P

HEAD = 256
THETA = 10000
NEG = -1e30
HIDDEN = 2 * NEG
LOG2E = 1.4426950408889634
E = HEAD**-0.5 * LOG2E
VMEM_MAX = 67043328
F32, BF16 = jnp.float32, jnp.bfloat16


def _dot(a, b, ca, cb):
    return lax.dot_general(a, b, (((ca,), (cb,)), ((), ())), preferred_element_type=F32)


SEMAPHORES = [(8, 0)] * 5 + [(2, 0)] * 3 + [(3, 5)] * 4 + [(1, 7)] * 4


def _layer(x_ref, gain_ref, freq_ref, wq_ref, wk_ref, wv_ref, wo_ref, y_ref, o_ref,
           a_s, cos_s, sin_s, q_s, k_s, v_s, rq, rk, rv, ro, lo, rl, wbuf, product_s, m_s, l_s, acc_s, total_s,
           x_sem, w_sem, wo_sem, st_sem, send_sem, recv_sem):
    me = lax.axis_index("sp")
    own, depth = a_s.shape
    heads = q_s.shape[0]
    groups = heads // 2
    half = own // 2
    wide = 2 * HEAD
    blocks = depth // wide

    P_END, W_FROM = 2, 5

    def flags(g):
        p, w = g < P_END, g >= W_FROM
        r = jnp.logical_not(p | w)
        pr = jnp.logical_not(w)
        d0, d1, d2, d3 = (me == d for d in range(4))
        return dict(
            send_q=(d2 & pr) | d3, q_to=jnp.where(d2, 1, jnp.where(w, 2, 0)), send_q2=d3 & p,
            send_kv=d0 | (d1 & pr) | (d2 & r), kv_to=jnp.where(d0, jnp.where(w, 3, 1), jnp.where(d1, 0, 3)),
            send_kv2=d1 & w, forward=w & (d2 | d3), forward_k=w & (d3 | (d2 & (g < groups - 1))), send_k1=d0 & (g == groups - 1),
            there=((d0 | d1) & pr) | (d2 & (p | w)), there_kv=(d0 | d1) & pr, there_kv2=d2 & w,
            send_o=((d0 | d1) & pr) | (d2 & w), o_to=jnp.where(d1, 2, 3), send_o1=d2 & p,
            await_kv=(d1 & w) | (d3 & r), await_k=d2 & (g == groups - 1), home_kv=d1 | (d2 & w) | (d3 & (r | w)), home_kv2=d2 & w,
            get_o=(d2 & pr) | d3, get_o1=d3 & p,
        )

    def two(ref, g):
        return ref.at[pl.ds(2 * g, 2)]

    def two_w(ref, g):
        return ref.at[pl.ds(2 * (g - W_FROM), 2)]

    def columns(g):
        return pl.ds(pl.multiple_of(g * wide, wide), wide)

    def place_of(kind, g):
        first = sum(n for n, _ in SEMAPHORES[:kind])
        return first + g - SEMAPHORES[kind][1]

    def remote(src, dst, kind, rkind, g, to):
        return pltpu.make_async_remote_copy(src_ref=src, dst_ref=dst, send_sem=send_sem.at[place_of(kind, g)], recv_sem=recv_sem.at[place_of(rkind, g)],
                                            device_id={"sp": to}, device_id_type=pl.DeviceIdType.MESH)

    def single(what, h, j, to):
        src, dst = ((q_s, rq), (rq, ro), (lo, rl))[what]
        kind = ((0, 12), (3, 13), (4, 14))[what][j]
        return remote(src.at[pl.ds(h + j, 1)], dst.at[pl.ds(h + j, 1)], kind, kind, groups - 1, to)

    last = groups - 1

    def copy(kind, g, f):
        return {
            0: lambda: remote(two(q_s, g), two(rq, g), 0, 0, g, f["q_to"]),
            1: lambda: remote(two(k_s, g), two(rk, g), 1, 1, g, f["kv_to"]),
            2: lambda: remote(two(v_s, g), two(rv, g), 2, 2, g, f["kv_to"]),
            3: lambda: remote(two(rq, g), two(ro, g), 3, 3, g, f["o_to"]),
            4: lambda: remote(two(lo, g), two(rl, g), 4, 4, g, f["o_to"]),
            5: lambda: remote(two(rq, g), two(rq, g), 5, 5, g, 3),
            6: lambda: remote(two(lo, g), two(lo, g), 6, 6, g, 3),
            7: lambda: remote(two(q_s, g), two(rq, g), 7, 0, g, 2),
            8: lambda: remote(two(k_s, g), two_w(rk, g), 8, 8, g, 2),
            9: lambda: remote(two(v_s, g), two(ro, g), 9, 9, g, 2),
            10: lambda: remote(two(rk, g), two(rk, g), 10, 1, g, me - 1),
            11: lambda: remote(two(rv, g), two(rv, g), 11, 2, g, me - 1),
            12: lambda: remote(two(k_s, g), two(rk, g), 15, 1, g, 1),
        }[kind]()

    Q, K, V = 0, 8, 16
    both = lambda *gs: [t + g for c in gs for t in (V, K) for g in (c if isinstance(c, tuple) else (c,))]
    queries = lambda *gs: [Q + g for g in gs]
    projections = [
        both((0, 5), (1, 6), (2, 7), 3, 4) + queries(0, 1, 2, 3, 4, 5, 6, 7),
        both((0, 5), (1, 6), (2, 7), 3, 4) + queries(0, 1, 2, 3, 4, 5, 6, 7),
        queries(0) + both(2) + queries(1, 2) + both(3) + queries(3, 4) + both(4, 0, 1, 5, 6, 7) + queries(5, 6, 7),
        queries(0, 1, 2, 3, 4, 5, 6, 7) + both(0, 1, 2, 3, 4, 5, 6, 7),
    ]
    homes = [[0, 1, 2, 3, 5, 6, 4, 7], [0, 1, 2, 3, 5, 6, 4, 7], [5, 6, 0, 1, 2, 3, 4, 7], [0, 1, 5, 2, 3, 6, 4, 7]]
    FWD, J, H, BEGIN, LATE, OWN = 8, 16, 17, 18, 24, 32
    Y, Z = OWN + groups - 1, OWN + groups - 4
    order = [
        [J] * 24 + [LATE + 7, 0, 1, BEGIN, 2, H, H, H, 3, H, H, H, 4, Z, H, Y, H],
        [J] * 24 + [0, 1, BEGIN, 2, H, H, H, 3, H, H, H, 4, Z, H, Y, H],
        [J] * 15 + [0, 1] + [J] * 7 + [FWD + 5] + [J] * 2 + [5, BEGIN, H, FWD + 6, H, H, 6, H, H, FWD + 7, 7, H, Z, Y, H, H],
        [J] * 11 + [FWD + 5] + [J] * 9 + [FWD + 6] + [J] * 4 + [LATE + 6, BEGIN, FWD + 7, LATE + 7, Y, H, H, H, H, H, H, Z, H, H],
    ]
    steps = max(len(o) for o in order)
    order = [o + [19] * (steps - len(o)) for o in order]

    def look(table, i):
        found = 0
        for n in range(len(table[0])):
            here = table[3][n]
            for d in range(3):
                if table[d][n] != table[3][n]:
                    here = jnp.where(me == d, table[d][n], here)
            found = jnp.where(i == n, here, found)
        return found

    def weights(what, slot, w):
        return pltpu.make_async_copy(w.at[:, columns(lax.rem(what, groups))], wbuf.at[slot], w_sem.at[slot])

    def fetch(i):
        what = look(projections, i)
        for t, w in enumerate((wq_ref, wk_ref, wv_ref)):
            @pl.when(lax.div(what, groups) == t)
            def _():
                weights(what, lax.rem(i, 3), w).start()

    def rows_in(r):
        return pltpu.make_async_copy(x_ref.at[pl.ds(r * (own // 4), own // 4)], a_s.at[pl.ds(r * (own // 4), own // 4)], x_sem.at[r])

    for r in range(4):
        rows_in(r).start()
    barrier = pltpu.get_barrier_semaphore()
    for n in (1, 2, 3):
        pl.semaphore_signal(barrier, inc=1, device_id={"sp": lax.rem(me + n, 4)}, device_id_type=pl.DeviceIdType.MESH)

    stretch = 32
    far = (me * own + stretch * lax.broadcasted_iota(jnp.int32, (own // stretch, HEAD // 2), 0)).astype(F32) * freq_ref[...]
    near = lax.broadcasted_iota(jnp.int32, (stretch, HEAD // 2), 0).astype(F32) * freq_ref[...]
    cos_far, sin_far, cos_near, sin_near = jnp.cos(far), jnp.sin(far), jnp.cos(near), jnp.sin(near)
    for n in range(own // stretch):
        c, d = cos_far[n : n + 1, :], sin_far[n : n + 1, :]
        cos_s[n * stretch : (n + 1) * stretch, :] = c * cos_near - d * sin_near
        sin_s[n * stretch : (n + 1) * stretch, :] = d * cos_near + c * sin_near

    gain = gain_ref[...].astype(F32)
    gain = jnp.concatenate([gain[n : n + 1, :] for n in range(depth // 128)], axis=1)
    for r in range(4):
        rows_in(r).wait()
        if r == 1:
            fetch(jnp.int32(0))
        at = slice(r * (own // 4), (r + 1) * (own // 4))
        x = a_s[at, :].astype(F32)
        scale = lax.rsqrt(jnp.mean(x * x, -1, keepdims=True) + 1e-6)
        a_s[at, :] = (a_s[at, :].astype(F32) * scale * gain).astype(BF16)

    for i in (1, 2):
        fetch(jnp.int32(i))
    pl.semaphore_wait(barrier, 3)

    def turned(part):
        full = part.astype(F32)
        x, y = full[:, : HEAD // 2], full[:, HEAD // 2 :]
        cos, sin = cos_s[...], sin_s[...]
        return jnp.concatenate([x * cos - y * sin, y * cos + x * sin], -1).astype(BF16)

    def project(i):
        what = look(projections, i)
        t, g = lax.div(what, groups), lax.rem(what, groups)
        h = 2 * g
        f = flags(g)
        slot = lax.rem(i, 3)
        weights(what, slot, wq_ref).wait()
        product_s[...] = _dot(a_s[...], wbuf[slot], 1, 0).astype(BF16)

        @pl.when(i + 3 < 3 * groups)
        def _():
            fetch(i + 3)

        @pl.when(t == 0)
        def _():
            for j in range(2):
                q_s[h + j] = turned(product_s[:, j * HEAD : (j + 1) * HEAD]).T
            late = (me == 3) & (g > W_FROM)
            for kind, on in ((0, "send_q"), (7, "send_q2")):
                @pl.when(f[on] & jnp.logical_not(late))
                def _():
                    copy(kind, g, f).start()

        @pl.when(t == 1)
        def _():
            for j in range(2):
                k_s[h + j] = turned(product_s[:, j * HEAD : (j + 1) * HEAD])

            for kind, on in ((1, "send_kv"), (8, "send_kv2")):
                @pl.when(f[on])
                def _():
                    copy(kind, g, f).start()

        @pl.when(t == 2)
        def _():
            for j in range(2):
                v_s[h + j] = product_s[:, j * HEAD : (j + 1) * HEAD].T

            for kind, on in ((2, "send_kv"), (9, "send_kv2")):
                @pl.when(f[on])
                def _():
                    copy(kind, g, f).start()

    def reset(st):
        m_s[st] = jnp.full(m_s.shape[1:], NEG, F32)
        l_s[st] = jnp.zeros(l_s.shape[1:], F32)
        acc_s[st] = jnp.zeros(acc_s.shape[1:], F32)

    def block(q, k, v, keys, queries, masked, js=(0, 1), st=0):
        scores = [_dot(k[j, keys, :], q[j, :, queries], 1, 0) for j in js]
        if masked:
            shape = scores[0].shape
            ok = (lax.broadcasted_iota(jnp.int32, shape, 1) + queries.start) >= (lax.broadcasted_iota(jnp.int32, shape, 0) + keys.start)
            scores = [jnp.where(ok, s, HIDDEN) for s in scores]
        ps, keeps = [], []
        for j, s in zip(js, scores):
            old = m_s[st, j, :, queries]
            top = jnp.maximum(old, s.max(axis=0, keepdims=True))
            p = jnp.exp2((s - top) * E)
            keep = jnp.exp2((old - top) * E)
            m_s[st, j, :, queries] = top
            l_s[st, j, :, queries] = l_s[st, j, :, queries] * keep + p.sum(axis=0, keepdims=True)
            ps.append(p.astype(BF16))
            keeps.append(keep)
        for j, p, keep in zip(js, ps, keeps):
            acc_s[st, j, :, queries] = acc_s[st, j, :, queries] * keep + _dot(v[j, :, keys], p, 1, 0)

    every = slice(0, own)

    def part(g, j):
        total = l_s[0, j]
        rq[2 * g + j] = (acc_s[0, j] * (1 / total)).astype(BF16)
        lo[2 * g + j] = m_s[0, j] * E + jnp.log2(total)

    def there_last():
        reset(0)
        for j in range(2):
            single(0, 2 * last, j, 2).wait_recv()
            block(two(rq, last), two(k_s, last), two(v_s, last), every, every, False, (j,))
            block(two(rq, last), two_w(rk, last), two(ro, last), every, every, False, (j,))
            part(last, j)
            single(1, 2 * last, j, 3).start()
            single(2, 2 * last, j, 3).start()

    def there(g):
        f = flags(g)

        @pl.when(f["there_kv"])
        def _():
            copy(1, g, f).wait_recv()
            copy(2, g, f).wait_recv()

        @pl.when(f["there"])
        def _():
            copy(0, g, f).wait_recv()
            reset(0)
            block(two(rq, g), two(k_s, g), two(v_s, g), every, every, False)

            @pl.when(f["there_kv"])
            def _():
                block(two(rq, g), two(rk, g), two(rv, g), every, every, False)

            @pl.when(f["there_kv2"])
            def _():
                block(two(rq, g), two_w(rk, g), two(ro, g), every, every, False)

            for j in range(2):
                part(g, j)

        for kind, on in ((3, "send_o"), (4, "send_o"), (5, "send_o1"), (6, "send_o1")):
            @pl.when(f[on])
            def _():
                copy(kind, g, f).start()

    def forward(g):
        f = flags(g)

        @pl.when((me == 3) | (g < last))
        def _():
            copy(10, g, f).wait_recv()

        copy(11, g, f).wait_recv()

        @pl.when(g < last)
        def _():
            copy(10, g, f).start()

        copy(11, g, f).start()

        @pl.when(me == 2)
        def _():
            copy(8, g, f).wait_recv()
            copy(9, g, f).wait_recv()

    def take(st, part, sums):
        for j in range(2):
            old, new = m_s[st, j], sums[j] * (1 / E)
            top = jnp.maximum(old, new)
            keep, add = jnp.exp2((old - top) * E), jnp.exp2((new - top) * E)
            m_s[st, j] = top
            l_s[st, j] = l_s[st, j] * keep + add
            acc_s[st, j] = acc_s[st, j] * keep + part[j].astype(F32) * add

    def early(g):
        return (g == last) | (g == groups - 4)

    def state(g):
        return (g == last).astype(jnp.int32)

    def share(g):
        f = flags(g)
        st = state(g)
        reset(st)
        q, k, v = two(q_s, g), two(k_s, g), two(v_s, g)
        block(q, k, v, slice(0, half), every, True, st=st)
        block(q, k, v, slice(half, own), slice(half, own), True, st=st)

        @pl.when(f["home_kv2"])
        def _():
            block(q, two_w(rk, g), two(ro, g), every, every, False, st=st)

        @pl.when(f["await_kv"])
        def _():
            copy(1, g, f).wait_recv()
            copy(2, g, f).wait_recv()

        @pl.when(f["await_k"])
        def _():
            copy(1, g, f).wait_recv()

        @pl.when(f["home_kv"])
        def _():
            block(q, two(rk, g), two(rv, g), every, every, False, st=st)

    def out_weights(i, n):
        slot = lax.rem(i, 3)
        return pltpu.make_async_copy(wo_ref.at[columns(look(homes, i)), pl.ds(pl.multiple_of(n * wide, wide), wide)],
                                     wbuf.at[slot, pl.ds(pl.multiple_of(n * wide, wide), wide)], wo_sem.at[slot, n])

    def residual(n):
        rows = pl.ds(pl.multiple_of(n * wide, wide), wide)
        return pltpu.make_async_copy(x_ref.at[:, rows], wbuf.at[2, rows], wo_sem.at[2, n])

    def fetch_out(i):
        lax.fori_loop(0, blocks, lambda n, _: out_weights(i, n).start(), None)

    def start_out():
        lax.fori_loop(0, blocks, lambda n, _: residual(n).start(), None)
        for i in range(2):
            fetch_out(i)

        def one(n, _):
            residual(n).wait()
            total_s[n] = wbuf[2, pl.ds(pl.multiple_of(n * wide, wide), wide), :].astype(F32)

        lax.fori_loop(0, blocks, one, None)
        fetch_out(2)

    def result(n):
        return pltpu.make_async_copy(total_s.at[n], y_ref.at[:, pl.ds(pl.multiple_of(n * wide, wide), wide)], st_sem.at[n])

    last_out = pltpu.make_async_copy(product_s, o_ref, x_sem.at[0])

    def home(i):
        g = look(homes, i)
        f = flags(g)
        st = state(g)

        @pl.when(jnp.logical_not(early(g)))
        def _():
            share(g)

        @pl.when(f["get_o"])
        def _():
            @pl.when(g < last)
            def _():
                copy(3, g, f).wait_recv()
                copy(4, g, f).wait_recv()

            @pl.when(g == last)
            def _():
                for j in range(2):
                    single(1, 2 * last, j, 3).wait_recv()
                    single(2, 2 * last, j, 3).wait_recv()

            take(st, two(ro, g), two(rl, g))

        @pl.when(f["get_o1"])
        def _():
            copy(5, g, f).wait_recv()
            copy(6, g, f).wait_recv()
            take(st, two(rq, g), two(lo, g))

        for j in range(2):
            product_s[:, j * HEAD : (j + 1) * HEAD] = (acc_s[st, j] * (1 / l_s[st, j])).T.astype(BF16)

        @pl.when(i == groups - 1)
        def _():
            last_out.start()

        @pl.when(i < groups - 1)
        def _():
            lax.fori_loop(0, blocks, lambda n, _: out_weights(i, n).wait(), None)
            slot = lax.rem(i, 3)
            for n in range(blocks):
                total_s[n] += _dot(product_s[...], wbuf[slot, n * wide : (n + 1) * wide, :], 1, 0)

                @pl.when(i == groups - 2)
                def _():
                    result(n).start()

            @pl.when(i + 3 < groups - 1)
            def _():
                fetch_out(i + 3)

    def step(t, done):
        projected, came = done
        what = look(order, t)

        @pl.when(what == J)
        def _():
            project(projected)

        @pl.when(what < last)
        def _():
            there(what)

        @pl.when(what == last)
        def _():
            there_last()

        @pl.when((what >= FWD) & (what < FWD + groups))
        def _():
            forward(what - FWD)

        @pl.when(what >= OWN)
        def _():
            share(what - OWN)

        @pl.when((what >= LATE) & (what < OWN))
        def _():
            g = what - LATE

            @pl.when(g < last)
            def _():
                copy(0, g, flags(g)).start()

            @pl.when((g == last) & (me == 3))
            def _():
                for j in range(2):
                    single(0, 2 * last, j, 2).start()
                copy(10, g, flags(g)).start()

            @pl.when((g == last) & (me == 0))
            def _():
                copy(12, g, flags(g)).start()

        @pl.when(what == BEGIN)
        def _():
            start_out()

        @pl.when(what == H)
        def _():
            home(came)

        return projected + (what == J).astype(jnp.int32), came + (what == H).astype(jnp.int32)

    lax.fori_loop(0, steps, step, (jnp.int32(0), jnp.int32(0)))
    lax.fori_loop(0, blocks, lambda n, _: result(n).wait(), None)
    last_out.wait()

    def drain(g, _):
        f = flags(g)
        for kind, on in ((0, "send_q"), (7, "send_q2"), (1, "send_kv"), (2, "send_kv"), (3, "send_o"), (4, "send_o"), (5, "send_o1"), (6, "send_o1"),
                         (8, "send_kv2"), (9, "send_kv2"), (10, "forward_k"), (11, "forward"), (12, "send_k1")):
            @pl.when(f[on] & (g < last if kind in (0, 3, 4) else True))
            def _():
                copy(kind, g, f).wait_send()

    lax.fori_loop(0, groups, drain, None)
    for j in range(2):
        @pl.when(me == 3)
        def _():
            single(0, 2 * last, j, 2).wait_send()

        @pl.when(me == 2)
        def _():
            single(1, 2 * last, j, 3).wait_send()
            single(2, 2 * last, j, 3).wait_send()


def layer(x, gain, freq, wq, wk, wv, wo):
    own, depth = x.shape
    heads = wq.shape[1] // HEAD
    groups = heads // 2
    vmem, hbm = pl.BlockSpec(memory_space=pltpu.VMEM), pl.BlockSpec(memory_space=pl.ANY)
    block = pltpu.VMEM((heads, own, HEAD), BF16)
    turned = pltpu.VMEM((heads, HEAD, own), BF16)
    sums = pltpu.VMEM((heads, 1, own), F32)
    wide = 2 * HEAD
    return pl.pallas_call(
        _layer,
        out_shape=[jax.ShapeDtypeStruct((own, depth), F32), jax.ShapeDtypeStruct((own, wide), BF16)],
        in_specs=[hbm, vmem, vmem, hbm, hbm, hbm, hbm],
        out_specs=[hbm, hbm],
        scratch_shapes=[
            pltpu.VMEM((own, depth), BF16), pltpu.VMEM((own, HEAD // 2), F32), pltpu.VMEM((own, HEAD // 2), F32),
            turned, block, turned, turned, block, turned,
            turned, sums, sums,
            pltpu.VMEM((3, depth, wide), BF16), pltpu.VMEM((own, wide), BF16),
            pltpu.VMEM((2, 2, 1, own), F32), pltpu.VMEM((2, 2, 1, own), F32), pltpu.VMEM((2, 2, HEAD, own), F32),
            pltpu.VMEM((depth // wide, own, wide), F32),
            pltpu.SemaphoreType.DMA((4,)), pltpu.SemaphoreType.DMA((3,)), pltpu.SemaphoreType.DMA((3, depth // wide)), pltpu.SemaphoreType.DMA((depth // wide,)),
            pltpu.SemaphoreType.DMA((sum(n for n, _ in SEMAPHORES),)), pltpu.SemaphoreType.DMA((sum(n for n, _ in SEMAPHORES[:15]),)),
        ],
        compiler_params=pltpu.CompilerParams(collective_id=0, has_side_effects=True, vmem_limit_bytes=VMEM_MAX),
        name="layer",
    )(x, gain, freq, wq, wk, wv, wo)


LAST_HOME = 7


def _finish(t_ref, o_ref, w_ref, y_ref):
    y_ref[...] = (t_ref[...] + _dot(o_ref[...], w_ref[...], 1, 0)).astype(BF16)


def finish(total, o, wo):
    own, depth = total.shape
    deep = o.shape[1]
    wide = depth // 2
    return pl.pallas_call(
        _finish,
        grid=(depth // wide,),
        in_specs=[pl.BlockSpec((own, wide), lambda n: (0, n)), pl.BlockSpec((own, deep), lambda n: (0, 0)), pl.BlockSpec((deep, wide), lambda n: (LAST_HOME, n))],
        out_specs=pl.BlockSpec((own, wide), lambda n: (0, n)),
        out_shape=jax.ShapeDtypeStruct((own, depth), BF16),
        compiler_params=pltpu.CompilerParams(dimension_semantics=("arbitrary",), vmem_limit_bytes=VMEM_MAX),
        name="finish",
    )(total, o, wo)


def solution(mesh):
    def step(x, gain, wq, wk, wv, wo):
        freq = np.float32(THETA) ** (-np.arange(HEAD // 2, dtype=np.float32) / np.float32(HEAD // 2))
        total, o = layer(x, gain.reshape(-1, 128), jnp.asarray(freq)[None], wq, wk, wv, wo)
        return finish(total, o, wo)

    tokens, whole = P(("dp", "sp"), None), P(None, None)
    return jax.shard_map(step, mesh=mesh, in_specs=(tokens, P(None), whole, whole, whole, whole), out_specs=tokens, check_vma=False)
```

```python
import jax
import jax.numpy as jnp
import numpy as np
from jax import lax
from jax.experimental import pallas as pl
from jax.experimental.pallas import tpu as pltpu
from jax.sharding import PartitionSpec as P

HEAD = 256
THETA = 10000
NEG = -1e30
HIDDEN = 2 * NEG
LOG2E = 1.4426950408889634
E = HEAD**-0.5 * LOG2E
VMEM_MAX = 67043328
F32, BF16 = jnp.float32, jnp.bfloat16


def _dot(a, b, ca, cb):
    return lax.dot_general(a, b, (((ca,), (cb,)), ((), ())), preferred_element_type=F32)


SEMAPHORES = [(8, 0)] * 5 + [(2, 0)] * 3 + [(3, 5)] * 4 + [(1, 7)] * 4 + [(1, 4)] * 2


def _layer(x_ref, gain_in, freq_in, wq_ref, wk_ref, wv_ref, wo_ref, y_ref, o_ref,
           gain_ref, freq_ref, a_s, cos_s, sin_s, q_s, k_s, v_s, rq, rk, rv, ro, lo, rl, wbuf, product_s, m_s, l_s, acc_s, total_s,
           in_sem, x_sem, w_sem, wo_sem, st_sem, send_sem, recv_sem):
    me = lax.axis_index("sp")
    own, depth = a_s.shape
    heads = q_s.shape[0]
    groups = heads // 2
    half = own // 2
    wide = 2 * HEAD
    blocks = depth // wide

    P_END, W_FROM = 2, 5

    def flags(g):
        p, w = g < P_END, g >= W_FROM
        r = jnp.logical_not(p | w)
        pr = jnp.logical_not(w)
        d0, d1, d2, d3 = (me == d for d in range(4))
        return dict(
            send_q=(d2 & pr) | d3, q_to=jnp.where(d2, 1, jnp.where(w, 2, 0)), send_q2=d3 & p,
            send_kv=d0 | (d1 & pr) | (d2 & r), kv_to=jnp.where(d0, jnp.where(w, 3, 1), jnp.where(d1, 0, 3)),
            send_kv2=d1 & w, forward=w & (d2 | d3), forward_k=w & (d3 | (d2 & (g < groups - 1))), send_k1=d0 & (g == groups - 1),
            there=((d0 | d1) & pr) | (d2 & (p | w)), there_kv=(d0 | d1) & pr, there_kv2=d2 & w,
            send_o=((d0 | d1) & pr) | (d2 & w), o_to=jnp.where(d1, 2, 3), send_o1=d2 & p,
            await_kv=(d1 & w) | (d3 & r), await_k=d2 & (g == groups - 1), home_kv=d1 | (d2 & w) | (d3 & (r | w)), home_kv2=d2 & w,
            get_o=(d2 & pr) | d3, get_o1=d3 & p,
        )

    def two(ref, g):
        return ref.at[pl.ds(2 * g, 2)]

    def two_w(ref, g):
        return ref.at[pl.ds(2 * (g - W_FROM), 2)]

    def columns(g):
        return pl.ds(pl.multiple_of(g * wide, wide), wide)

    def place_of(kind, g):
        first = sum(n for n, _ in SEMAPHORES[:kind])
        return first + g - SEMAPHORES[kind][1]

    def remote(src, dst, kind, rkind, g, to):
        return pltpu.make_async_remote_copy(src_ref=src, dst_ref=dst, send_sem=send_sem.at[place_of(kind, g)], recv_sem=recv_sem.at[place_of(rkind, g)],
                                            device_id={"sp": to}, device_id_type=pl.DeviceIdType.MESH)

    def single(what, g, j, to):
        src, dst = ((q_s, rq), (rq, ro), (lo, rl))[what]
        kind = (((0, 12), (3, 13), (4, 14)) if g == last else ((), (3, 16), (4, 17)))[what][j]
        return remote(src.at[pl.ds(2 * g + j, 1)], dst.at[pl.ds(2 * g + j, 1)], kind, kind, g, to)

    last, near_last = groups - 1, groups - 4

    def copy(kind, g, f):
        return {
            0: lambda: remote(two(q_s, g), two(rq, g), 0, 0, g, f["q_to"]),
            1: lambda: remote(two(k_s, g), two(rk, g), 1, 1, g, f["kv_to"]),
            2: lambda: remote(two(v_s, g), two(rv, g), 2, 2, g, f["kv_to"]),
            3: lambda: remote(two(rq, g), two(ro, g), 3, 3, g, f["o_to"]),
            4: lambda: remote(two(lo, g), two(rl, g), 4, 4, g, f["o_to"]),
            5: lambda: remote(two(rq, g), two(rq, g), 5, 5, g, 3),
            6: lambda: remote(two(lo, g), two(lo, g), 6, 6, g, 3),
            7: lambda: remote(two(q_s, g), two(rq, g), 7, 0, g, 2),
            8: lambda: remote(two(k_s, g), two_w(rk, g), 8, 8, g, 2),
            9: lambda: remote(two(v_s, g), two(ro, g), 9, 9, g, 2),
            10: lambda: remote(two(rk, g), two(rk, g), 10, 1, g, me - 1),
            11: lambda: remote(two(rv, g), two(rv, g), 11, 2, g, me - 1),
            12: lambda: remote(two(k_s, g), two(rk, g), 15, 1, g, 1),
        }[kind]()

    Q, K, V = 0, 8, 16
    both = lambda *gs: [t + g for c in gs for t in (V, K) for g in (c if isinstance(c, tuple) else (c,))]
    queries = lambda *gs: [Q + g for g in gs]
    projections = [
        both((0, 5), (1, 6), (2, 7), 3, 4) + queries(0, 1, 2, 3, 4, 5, 6, 7),
        both((0, 5), (1, 6), (2, 7), 3, 4) + queries(0, 1, 2, 3, 4, 5, 6, 7),
        [V + 2] + queries(0) + [K + 2] + queries(1, 2) + both(3) + queries(3, 4) + both(4, 0, 1, 5, 6, 7) + queries(5, 6, 7),
        queries(0, 1, 2, 3, 4, 5, 6, 7) + both(0, 1, 2, 3, 4, 5, 6, 7),
    ]
    homes = [[0, 1, 2, 3, 5, 6, 4, 7], [0, 1, 2, 3, 5, 6, 4, 7], [5, 6, 0, 1, 2, 3, 4, 7], [0, 1, 5, 2, 3, 6, 4, 7]]
    FWD, J, H, BEGIN, LATE, OWN = 8, 16, 17, 18, 24, 32
    Y, Z = OWN + groups - 1, OWN + groups - 4
    order = [
        [J] * 24 + [LATE + 7, 0, 1, BEGIN, 2, H, H, H, 3, H, H, H, 4, Z, H, Y, H],
        [J] * 24 + [0, 1, BEGIN, 2, H, H, H, 3, H, H, H, 4, Z, H, Y, H],
        [J] * 15 + [0, 1] + [J] * 7 + [FWD + 5] + [J] * 2 + [5, BEGIN, H, FWD + 6, H, H, 6, H, H, FWD + 7, 7, H, Z, Y, H, H],
        [J] * 11 + [FWD + 5] + [J] * 9 + [FWD + 6] + [J] * 4 + [LATE + 6, BEGIN, FWD + 7, LATE + 7, Y, H, H, H, H, H, H, Z, H, H],
    ]
    steps = max(len(o) for o in order)
    order = [o + [19] * (steps - len(o)) for o in order]

    def look(table, i):
        found = 0
        for n in range(len(table[0])):
            here = table[3][n]
            for d in range(3):
                if table[d][n] != table[3][n]:
                    here = jnp.where(me == d, table[d][n], here)
            found = jnp.where(i == n, here, found)
        return found

    def weights(what, slot, w):
        return pltpu.make_async_copy(w.at[:, columns(lax.rem(what, groups))], wbuf.at[slot], w_sem.at[slot])

    def fetch(i):
        what = look(projections, i)
        for t, w in enumerate((wq_ref, wk_ref, wv_ref)):
            @pl.when(lax.div(what, groups) == t)
            def _():
                weights(what, lax.rem(i, 3), w).start()

    def rows_in(r):
        return pltpu.make_async_copy(x_ref.at[pl.ds(r * (own // 4), own // 4)], a_s.at[pl.ds(r * (own // 4), own // 4)], x_sem.at[r])

    for r in range(4):
        rows_in(r).start()
    small = [pltpu.make_async_copy(a, b, in_sem.at[n]) for n, (a, b) in enumerate(((freq_in, freq_ref), (gain_in, gain_ref)))]
    for one in small:
        one.start()

    barrier = pltpu.get_barrier_semaphore()
    for n in (1, 2, 3):
        pl.semaphore_signal(barrier, inc=1, device_id={"sp": lax.rem(me + n, 4)}, device_id_type=pl.DeviceIdType.MESH)

    small[0].wait()
    stretch = 32
    far = (me * own + stretch * lax.broadcasted_iota(jnp.int32, (own // stretch, HEAD // 2), 0)).astype(F32) * freq_ref[...]
    near = lax.broadcasted_iota(jnp.int32, (stretch, HEAD // 2), 0).astype(F32) * freq_ref[...]
    cos_far, sin_far, cos_near, sin_near = jnp.cos(far), jnp.sin(far), jnp.cos(near), jnp.sin(near)
    for n in range(own // stretch):
        c, d = cos_far[n : n + 1, :], sin_far[n : n + 1, :]
        cos_s[n * stretch : (n + 1) * stretch, :] = c * cos_near - d * sin_near
        sin_s[n * stretch : (n + 1) * stretch, :] = d * cos_near + c * sin_near

    small[1].wait()
    gain = gain_ref[...].astype(F32)
    gain = jnp.concatenate([gain[n : n + 1, :] for n in range(depth // 128)], axis=1)
    for r in range(4):
        rows_in(r).wait()
        if r == 1:
            fetch(jnp.int32(0))
        at = slice(r * (own // 4), (r + 1) * (own // 4))
        x = a_s[at, :].astype(F32)
        scale = lax.rsqrt(jnp.mean(x * x, -1, keepdims=True) + 1e-6)
        a_s[at, :] = (a_s[at, :].astype(F32) * scale * gain).astype(BF16)

    for i in (1, 2):
        fetch(jnp.int32(i))
    pl.semaphore_wait(barrier, 3)

    def turned(part):
        full = part.astype(F32)
        x, y = full[:, : HEAD // 2], full[:, HEAD // 2 :]
        cos, sin = cos_s[...], sin_s[...]
        return jnp.concatenate([x * cos - y * sin, y * cos + x * sin], -1).astype(BF16)

    def project(i):
        what = look(projections, i)
        t, g = lax.div(what, groups), lax.rem(what, groups)
        h = 2 * g
        f = flags(g)
        slot = lax.rem(i, 3)
        weights(what, slot, wq_ref).wait()
        product_s[...] = _dot(a_s[...], wbuf[slot], 1, 0).astype(BF16)

        @pl.when(i + 3 < 3 * groups)
        def _():
            fetch(i + 3)

        @pl.when(t == 0)
        def _():
            for j in range(2):
                q_s[h + j] = turned(product_s[:, j * HEAD : (j + 1) * HEAD]).T
            late = (me == 3) & (g > W_FROM)
            for kind, on in ((0, "send_q"), (7, "send_q2")):
                @pl.when(f[on] & jnp.logical_not(late))
                def _():
                    copy(kind, g, f).start()

        @pl.when(t == 1)
        def _():
            for j in range(2):
                k_s[h + j] = turned(product_s[:, j * HEAD : (j + 1) * HEAD])

            for kind, on in ((1, "send_kv"), (8, "send_kv2")):
                @pl.when(f[on])
                def _():
                    copy(kind, g, f).start()

        @pl.when(t == 2)
        def _():
            for j in range(2):
                v_s[h + j] = product_s[:, j * HEAD : (j + 1) * HEAD].T

            for kind, on in ((2, "send_kv"), (9, "send_kv2")):
                @pl.when(f[on])
                def _():
                    copy(kind, g, f).start()

    def reset(st):
        m_s[st] = jnp.full(m_s.shape[1:], NEG, F32)
        l_s[st] = jnp.zeros(l_s.shape[1:], F32)
        acc_s[st] = jnp.zeros(acc_s.shape[1:], F32)

    def block(q, k, v, keys, queries, masked, js=(0, 1), st=0):
        scores = [_dot(k[j, keys, :], q[j, :, queries], 1, 0) for j in js]
        if masked:
            shape = scores[0].shape
            ok = (lax.broadcasted_iota(jnp.int32, shape, 1) + queries.start) >= (lax.broadcasted_iota(jnp.int32, shape, 0) + keys.start)
            scores = [jnp.where(ok, s, HIDDEN) for s in scores]
        ps, keeps = [], []
        for j, s in zip(js, scores):
            old = m_s[st, j, :, queries]
            top = jnp.maximum(old, s.max(axis=0, keepdims=True))
            p = jnp.exp2((s - top) * E)
            keep = jnp.exp2((old - top) * E)
            m_s[st, j, :, queries] = top
            l_s[st, j, :, queries] = l_s[st, j, :, queries] * keep + p.sum(axis=0, keepdims=True)
            ps.append(p.astype(BF16))
            keeps.append(keep)
        for j, p, keep in zip(js, ps, keeps):
            acc_s[st, j, :, queries] = acc_s[st, j, :, queries] * keep + _dot(v[j, :, keys], p, 1, 0)

    every = slice(0, own)

    def part(g, j):
        total = l_s[0, j]
        rq[2 * g + j] = (acc_s[0, j] * (1 / total)).astype(BF16)
        lo[2 * g + j] = m_s[0, j] * E + jnp.log2(total)

    def there_last():
        reset(0)
        for j in range(2):
            single(0, last, j, 2).wait_recv()
            block(two(rq, last), two(k_s, last), two(v_s, last), every, every, False, (j,))
            block(two(rq, last), two_w(rk, last), two(ro, last), every, every, False, (j,))
            part(last, j)
            single(1, last, j, 3).start()
            single(2, last, j, 3).start()

    def there_near_last():
        f = flags(jnp.int32(near_last))
        copy(1, near_last, f).wait_recv()
        copy(2, near_last, f).wait_recv()
        copy(0, near_last, f).wait_recv()
        reset(0)
        q, k, v, k2, v2 = (two(ref, near_last) for ref in (rq, k_s, v_s, rk, rv))
        for j in range(2):
            block(q, k, v, every, every, False, (j,))
            block(q, k2, v2, every, every, False, (j,))
            part(near_last, j)
            single(1, near_last, j, f["o_to"]).start()
            single(2, near_last, j, f["o_to"]).start()

    def there(g):
        f = flags(g)

        @pl.when(f["there_kv"])
        def _():
            copy(1, g, f).wait_recv()
            copy(2, g, f).wait_recv()

        @pl.when(f["there"])
        def _():
            copy(0, g, f).wait_recv()
            reset(0)
            block(two(rq, g), two(k_s, g), two(v_s, g), every, every, False)

            @pl.when(f["there_kv"])
            def _():
                block(two(rq, g), two(rk, g), two(rv, g), every, every, False)

            @pl.when(f["there_kv2"])
            def _():
                block(two(rq, g), two_w(rk, g), two(ro, g), every, every, False)

            for j in range(2):
                part(g, j)

        for kind, on in ((3, "send_o"), (4, "send_o"), (5, "send_o1"), (6, "send_o1")):
            @pl.when(f[on])
            def _():
                copy(kind, g, f).start()

    def forward(g):
        f = flags(g)

        @pl.when((me == 3) | (g < last))
        def _():
            copy(10, g, f).wait_recv()

        copy(11, g, f).wait_recv()

        @pl.when(g < last)
        def _():
            copy(10, g, f).start()

        copy(11, g, f).start()

        @pl.when(me == 2)
        def _():
            copy(8, g, f).wait_recv()
            copy(9, g, f).wait_recv()

    def take(st, part, sums):
        for j in range(2):
            old, new = m_s[st, j], sums[j] * (1 / E)
            top = jnp.maximum(old, new)
            keep, add = jnp.exp2((old - top) * E), jnp.exp2((new - top) * E)
            m_s[st, j] = top
            l_s[st, j] = l_s[st, j] * keep + add
            acc_s[st, j] = acc_s[st, j] * keep + part[j].astype(F32) * add

    def early(g):
        return (g == last) | (g == groups - 4)

    def state(g):
        return (g == last).astype(jnp.int32)

    def share(g):
        f = flags(g)
        st = state(g)
        reset(st)
        q, k, v = two(q_s, g), two(k_s, g), two(v_s, g)
        block(q, k, v, slice(0, half), every, True, st=st)
        block(q, k, v, slice(half, own), slice(half, own), True, st=st)

        @pl.when(f["home_kv2"])
        def _():
            block(q, two_w(rk, g), two(ro, g), every, every, False, st=st)

        @pl.when(f["await_kv"])
        def _():
            copy(1, g, f).wait_recv()
            copy(2, g, f).wait_recv()

        @pl.when(f["await_k"])
        def _():
            copy(1, g, f).wait_recv()

        @pl.when(f["home_kv"])
        def _():
            block(q, two(rk, g), two(rv, g), every, every, False, st=st)

    def out_weights(i, n):
        slot = lax.rem(i, 3)
        return pltpu.make_async_copy(wo_ref.at[columns(look(homes, i)), pl.ds(pl.multiple_of(n * wide, wide), wide)],
                                     wbuf.at[slot, pl.ds(pl.multiple_of(n * wide, wide), wide)], wo_sem.at[slot, n])

    def residual(n):
        rows = pl.ds(pl.multiple_of(n * wide, wide), wide)
        return pltpu.make_async_copy(x_ref.at[:, rows], wbuf.at[2, rows], wo_sem.at[2, n])

    def fetch_out(i):
        lax.fori_loop(0, blocks, lambda n, _: out_weights(i, n).start(), None)

    def start_out():
        lax.fori_loop(0, blocks, lambda n, _: residual(n).start(), None)
        for i in range(2):
            fetch_out(i)

        def one(n, _):
            residual(n).wait()
            total_s[n] = wbuf[2, pl.ds(pl.multiple_of(n * wide, wide), wide), :].astype(F32)

        lax.fori_loop(0, blocks, one, None)
        fetch_out(2)

    def result(n):
        return pltpu.make_async_copy(total_s.at[n], y_ref.at[:, pl.ds(pl.multiple_of(n * wide, wide), wide)], st_sem.at[n])

    last_out = pltpu.make_async_copy(product_s, o_ref, x_sem.at[0])

    def home(i):
        g = look(homes, i)
        f = flags(g)
        st = state(g)

        @pl.when(jnp.logical_not(early(g)))
        def _():
            share(g)

        @pl.when(f["get_o"])
        def _():
            @pl.when((g < last) & (g != near_last))
            def _():
                copy(3, g, f).wait_recv()
                copy(4, g, f).wait_recv()

            for one in (near_last, last):
                @pl.when(g == one)
                def _():
                    for j in range(2):
                        single(1, one, j, 3).wait_recv()
                        single(2, one, j, 3).wait_recv()

            take(st, two(ro, g), two(rl, g))

        @pl.when(f["get_o1"])
        def _():
            copy(5, g, f).wait_recv()
            copy(6, g, f).wait_recv()
            take(st, two(rq, g), two(lo, g))

        for j in range(2):
            product_s[:, j * HEAD : (j + 1) * HEAD] = (acc_s[st, j] * (1 / l_s[st, j])).T.astype(BF16)

        @pl.when(i == groups - 1)
        def _():
            last_out.start()

        @pl.when(i < groups - 1)
        def _():
            lax.fori_loop(0, blocks, lambda n, _: out_weights(i, n).wait(), None)
            slot = lax.rem(i, 3)
            for n in range(blocks):
                total_s[n] += _dot(product_s[...], wbuf[slot, n * wide : (n + 1) * wide, :], 1, 0)

                @pl.when(i == groups - 2)
                def _():
                    result(n).start()

            @pl.when(i + 3 < groups - 1)
            def _():
                fetch_out(i + 3)

    def step(t, done):
        projected, came = done
        what = look(order, t)

        @pl.when(what == J)
        def _():
            project(projected)

        @pl.when((what < last) & (what != near_last))
        def _():
            there(what)

        @pl.when(what == near_last)
        def _():
            there_near_last()

        @pl.when(what == last)
        def _():
            there_last()

        @pl.when((what >= FWD) & (what < FWD + groups))
        def _():
            forward(what - FWD)

        @pl.when(what >= OWN)
        def _():
            share(what - OWN)

        @pl.when((what >= LATE) & (what < OWN))
        def _():
            g = what - LATE

            @pl.when(g < last)
            def _():
                copy(0, g, flags(g)).start()

            @pl.when((g == last) & (me == 3))
            def _():
                for j in range(2):
                    single(0, last, j, 2).start()
                copy(10, g, flags(g)).start()

            @pl.when((g == last) & (me == 0))
            def _():
                copy(12, g, flags(g)).start()

        @pl.when(what == BEGIN)
        def _():
            start_out()

        @pl.when(what == H)
        def _():
            home(came)

        return projected + (what == J).astype(jnp.int32), came + (what == H).astype(jnp.int32)

    lax.fori_loop(0, steps, step, (jnp.int32(0), jnp.int32(0)))
    lax.fori_loop(0, blocks, lambda n, _: result(n).wait(), None)
    last_out.wait()

    def drain(g, _):
        f = flags(g)
        for kind, on in ((0, "send_q"), (7, "send_q2"), (1, "send_kv"), (2, "send_kv"), (3, "send_o"), (4, "send_o"), (5, "send_o1"), (6, "send_o1"),
                         (8, "send_kv2"), (9, "send_kv2"), (10, "forward_k"), (11, "forward"), (12, "send_k1")):
            @pl.when(f[on] & (g < last if kind == 0 else (g < last) & (g != near_last) if kind in (3, 4) else True))
            def _():
                copy(kind, g, f).wait_send()

    lax.fori_loop(0, groups, drain, None)
    for j in range(2):
        @pl.when(me < 2)
        def _():
            single(1, near_last, j, 3 - me).wait_send()
            single(2, near_last, j, 3 - me).wait_send()

        @pl.when(me == 3)
        def _():
            single(0, last, j, 2).wait_send()

        @pl.when(me == 2)
        def _():
            single(1, last, j, 3).wait_send()
            single(2, last, j, 3).wait_send()


def layer(x, gain, freq, wq, wk, wv, wo):
    own, depth = x.shape
    heads = wq.shape[1] // HEAD
    groups = heads // 2
    hbm = pl.BlockSpec(memory_space=pl.ANY)
    block = pltpu.VMEM((heads, own, HEAD), BF16)
    turned = pltpu.VMEM((heads, HEAD, own), BF16)
    sums = pltpu.VMEM((heads, 1, own), F32)
    wide = 2 * HEAD
    return pl.pallas_call(
        _layer,
        out_shape=[jax.ShapeDtypeStruct((own, depth), F32), jax.ShapeDtypeStruct((own, wide), BF16)],
        in_specs=[hbm] * 7,
        out_specs=[hbm, hbm],
        scratch_shapes=[
            pltpu.VMEM(gain.shape, gain.dtype), pltpu.VMEM(freq.shape, freq.dtype), pltpu.VMEM((own, depth), BF16), pltpu.VMEM((own, HEAD // 2), F32), pltpu.VMEM((own, HEAD // 2), F32),
            turned, block, turned, turned, block, turned,
            turned, sums, sums,
            pltpu.VMEM((3, depth, wide), BF16), pltpu.VMEM((own, wide), BF16),
            pltpu.VMEM((2, 2, 1, own), F32), pltpu.VMEM((2, 2, 1, own), F32), pltpu.VMEM((2, 2, HEAD, own), F32),
            pltpu.VMEM((depth // wide, own, wide), F32),
            pltpu.SemaphoreType.DMA((2,)), pltpu.SemaphoreType.DMA((4,)), pltpu.SemaphoreType.DMA((3,)), pltpu.SemaphoreType.DMA((3, depth // wide)), pltpu.SemaphoreType.DMA((depth // wide,)),
            pltpu.SemaphoreType.DMA((sum(n for n, _ in SEMAPHORES),)), pltpu.SemaphoreType.DMA((sum(n for n, _ in SEMAPHORES),)),
        ],
        compiler_params=pltpu.CompilerParams(collective_id=0, has_side_effects=True, vmem_limit_bytes=VMEM_MAX),
        name="layer",
    )(x, gain, freq, wq, wk, wv, wo)


LAST_HOME = 7


def _finish(t_ref, o_ref, w_ref, y_ref):
    y_ref[...] = (t_ref[...] + _dot(o_ref[...], w_ref[...], 1, 0)).astype(BF16)


def finish(total, o, wo):
    own, depth = total.shape
    deep = o.shape[1]
    wide = depth // 2
    return pl.pallas_call(
        _finish,
        grid=(depth // wide,),
        in_specs=[pl.BlockSpec((own, wide), lambda n: (0, n)), pl.BlockSpec((own, deep), lambda n: (0, 0)), pl.BlockSpec((deep, wide), lambda n: (LAST_HOME, n))],
        out_specs=pl.BlockSpec((own, wide), lambda n: (0, n)),
        out_shape=jax.ShapeDtypeStruct((own, depth), BF16),
        compiler_params=pltpu.CompilerParams(dimension_semantics=("arbitrary",), vmem_limit_bytes=VMEM_MAX),
        name="finish",
    )(total, o, wo)


def solution(mesh):
    def step(x, gain, wq, wk, wv, wo):
        freq = np.float32(THETA) ** (-np.arange(HEAD // 2, dtype=np.float32) / np.float32(HEAD // 2))
        total, o = layer(x, gain.reshape(-1, 128), jnp.asarray(freq)[None], wq, wk, wv, wo)
        return finish(total, o, wo)

    tokens, whole = P(("dp", "sp"), None), P(None, None)
    return jax.shard_map(step, mesh=mesh, in_specs=(tokens, P(None), whole, whole, whole, whole), out_specs=tokens, check_vma=False)
```
